128 devices in a mesh: head: 8 (over z, y_lo), pts: 16 (over y_hi, x, core).
Axes of the slice: x: 4, y: 4 (y_hi: 2, y_lo: 2; y = y_hi * 2 + y_lo), z: 4, core: 2. Of those that a mesh axis runs over, the one named last changes fastest.
Arguments:
- layer_inputs_trainorder: bfloat16 [786432, 256], P(('head', 'pts')), may hold values from -6 to 6
- inference_placement: int32 [786432], P(('head', 'pts')), may hold values from 0 to 786431, as said below
- initial_layernorm_gain: float32 [256], replicated, may hold values from 0.1 to 1.9
- initial_layernorm_offset: float32 [256], replicated, may hold values from -2 to 2
- attribute_projection: bfloat16 [256, 256], replicated, may hold values from -0.375 to 0.375
- assignment_feeder_projection: bfloat16 [256, 256], replicated, may hold values from -0.375 to 0.375
- partition_projection: bfloat16 [16, 32], replicated, may hold values from -1.5 to 1.5
- partition_offset: float32 [32], replicated, may hold values from -4 to 4
- softmax_sharpness: float32 [16], P('head'), may hold values from 0.03 to 1
- partition_question_map: float32 [16, 16], replicated, may hold values from -1.5 to 1.5
- partition_lookup_map: float32 [16, 16], replicated, may hold values from -1.5 to 1.5
- partition_content_map: float32 [16, 16], replicated, may hold values from -1.5 to 1.5
- emitted_projection: bfloat16 [256, 256], replicated, may hold values from -0.375 to 0.375
- emitted_offset: float32 [256], replicated, may hold values from -2 to 2
- latter_layernorm_gain: float32 [256], replicated, may hold values from 0.1 to 1.9
- latter_layernorm_offset: float32 [256], replicated, may hold values from -2 to 2
- perceptron_entry_map: bfloat16 [256, 1024], replicated, may hold values from -0.375 to 0.375
- perceptron_entry_offset: float32 [1024], replicated, may hold values from -2 to 2
- perceptron_exit_map: bfloat16 [1024, 256], replicated, may hold values from -0.1875 to 0.1875
- perceptron_exit_offset: float32 [256], replicated, may hold values from -2 to 2
Outputs:
- served: bfloat16 [16, 49152, 256], P('pts', 'head')
The draws below stay inside these ranges and needn't reach their ends.
Inputs may be any that keep to these rules, and one draw needn't show every extreme that they name: inference_placement is a permutation of all points; of the 6144 points of each aligned block of the training order, exactly 48 go to each aligned block of 6144 serving positions.
All inputs are finite; a program needn't handle non-finite values.
Results may differ from the reference program's by a relative error of at most 0.0035.
The reference program's roundings to bfloat16 on the way count: a program that leaves them out, or rounds other values in their place, can miss the bound.
Values may be sent and summed in bfloat16 or wider, within the bound.
A program may use at most 128 MiB of HBM per device.

```python
import math
import jax
import jax.numpy as jnp
from jax import lax

ATTENDER_TOTAL = 16
DH = 16
M = 32
FF = 1024
PTS_DEV = 6144
MODEL_CHANNELS = 256
SERVE = 49152
POINTS = 786432
N_PTS = 16


def draw_inference_placement(key, part):
    blocks = POINTS // PTS_DEV
    per_pair = PTS_DEV // blocks
    first_keys = jax.random.split(jax.random.fold_in(key, 11), blocks)
    second_keys = jax.random.split(jax.random.fold_in(key, 12), blocks)
    within = jax.vmap(lambda single: jax.random.permutation(single, PTS_DEV))(first_keys).astype(jnp.int32)
    arrival = jax.vmap(lambda single: jax.random.permutation(single, PTS_DEV))(second_keys).astype(jnp.int32)
    target = within // per_pair
    ranks_in = within % per_pair
    source_ids = jnp.arange(blocks, dtype=jnp.int32)[:, None]
    slot_ids = source_ids * per_pair + ranks_in
    positions = target * PTS_DEV + arrival[target, slot_ids]
    return positions.reshape(-1).astype(jnp.int32)


def level_of(key, shape, cuts, smallest, high):
    loudness, own = 1.0, jax.random.fold_in(key, 6)
    for axis_at, parts in cuts:
        steps = jnp.exp(jax.random.uniform(jax.random.fold_in(own, axis_at), (parts,), jnp.float32, smallest / len(cuts), high / len(cuts)))
        loudness = loudness * jnp.repeat(steps, shape[axis_at] // parts).reshape([-1 if axis == axis_at else 1 for axis in range(len(shape))])
    return loudness


def bell_draw(stream_key, shape, deviation, bound, cuts=(), held_as=jnp.bfloat16):
    loudness = level_of(stream_key, shape, cuts, -0.22, 0.18) if cuts else 1.0
    result = jax.random.normal(stream_key, shape, jnp.float32) * deviation * loudness
    return jnp.minimum(jnp.maximum(result, -bound), bound).astype(held_as)


def setup_inputs(seed: int = 0) -> dict:
    key_of = jax.random.split(jax.random.key(seed), 21)
    return {
        "layer_inputs_trainorder": bell_draw(key_of[0], (POINTS, MODEL_CHANNELS), 1.0, 6.0, ((0, 128),)),
        "inference_placement": draw_inference_placement(jax.random.fold_in(key_of[20], 71), 0),
        "initial_layernorm_gain": jnp.clip(1.0 + 0.18 * jax.random.normal(key_of[2], (MODEL_CHANNELS,), jnp.float32), 0.1, 1.9),
        "initial_layernorm_offset": bell_draw(key_of[3], (MODEL_CHANNELS,), 0.3, 2.0, (), jnp.float32),
        "attribute_projection": bell_draw(key_of[4], (MODEL_CHANNELS, MODEL_CHANNELS), MODEL_CHANNELS ** -0.5, 0.375),
        "assignment_feeder_projection": bell_draw(key_of[5], (MODEL_CHANNELS, MODEL_CHANNELS), MODEL_CHANNELS ** -0.5, 0.375),
        "partition_projection": bell_draw(key_of[6], (DH, M), DH ** -0.5, 1.5),
        "partition_offset": bell_draw(key_of[7], (M,), 1.0, 4.0, (), jnp.float32),
        "softmax_sharpness": jnp.clip(jnp.exp(math.log(1.0) - 3.506558 * jax.random.uniform(key_of[8], (ATTENDER_TOTAL,), jnp.float32) ** level_of(key_of[8], (ATTENDER_TOTAL,), ((0, 8),), -0.2, 0.2)), 0.03, 1.0),
        "partition_question_map": bell_draw(key_of[9], (DH, DH), DH ** -0.5, 1.5, (), jnp.float32),
        "partition_lookup_map": bell_draw(key_of[10], (DH, DH), DH ** -0.5, 1.5, (), jnp.float32),
        "partition_content_map": bell_draw(key_of[11], (DH, DH), DH ** -0.5, 1.5, (), jnp.float32),
        "emitted_projection": bell_draw(key_of[12], (MODEL_CHANNELS, MODEL_CHANNELS), MODEL_CHANNELS ** -0.5, 0.375),
        "emitted_offset": bell_draw(key_of[13], (MODEL_CHANNELS,), 0.3, 2.0, (), jnp.float32),
        "latter_layernorm_gain": jnp.clip(1.0 + 0.18 * jax.random.normal(key_of[14], (MODEL_CHANNELS,), jnp.float32), 0.1, 1.9),
        "latter_layernorm_offset": bell_draw(key_of[15], (MODEL_CHANNELS,), 0.3, 2.0, (), jnp.float32),
        "perceptron_entry_map": bell_draw(key_of[16], (MODEL_CHANNELS, FF), MODEL_CHANNELS ** -0.5, 0.375),
        "perceptron_entry_offset": bell_draw(key_of[17], (FF,), 0.3, 2.0, (), jnp.float32),
        "perceptron_exit_map": bell_draw(key_of[18], (FF, MODEL_CHANNELS), FF ** -0.5, 0.1875),
        "perceptron_exit_offset": bell_draw(key_of[19], (MODEL_CHANNELS,), 0.3, 2.0, (), jnp.float32),
    }


def layer_norm(row_block, gain_vec, bias_vec):
    row_mean = lax.optimization_barrier(jnp.mean(row_block, axis=-1, keepdims=True))
    centred = row_block - row_mean
    spread = lax.optimization_barrier(jnp.mean(centred * centred, axis=-1, keepdims=True))
    return centred * lax.rsqrt(spread + 1e-05) * gain_vec + bias_vec

def truncated_coefficients(value):
    return lax.optimization_barrier(value.astype(jnp.bfloat16)).astype(jnp.float32)

def partition_share_entries(standardized_entries, assignment_feeder_projection, partition_projection, partition_offset, softmax_sharpness):
    middle = truncated_coefficients(jnp.dot(standardized_entries, assignment_feeder_projection, preferred_element_type=jnp.float32)).reshape(-1, ATTENDER_TOTAL, DH)
    partition_scores_raw = jnp.einsum('rhd,dm->rhm', middle, partition_projection.astype(jnp.float32))
    partition_scores_raw = (partition_scores_raw + partition_offset) / softmax_sharpness[:, None]
    return jax.nn.softmax(partition_scores_raw, axis=-1)

def reference(layer_inputs_trainorder, inference_placement, initial_layernorm_gain, initial_layernorm_offset, attribute_projection, assignment_feeder_projection, partition_projection, partition_offset, softmax_sharpness, partition_question_map, partition_lookup_map, partition_content_map, emitted_projection, emitted_offset, latter_layernorm_gain, latter_layernorm_offset, perceptron_entry_map, perceptron_entry_offset, perceptron_exit_map, perceptron_exit_offset):
    block_count = POINTS // PTS_DEV
    row_blocks = layer_inputs_trainorder.reshape(block_count, PTS_DEV, MODEL_CHANNELS)

    def gather_sums(running_state, row_block):
        standardized_entries = layer_norm(row_block.astype(jnp.float32), initial_layernorm_gain, initial_layernorm_offset).astype(jnp.bfloat16)
        slice_feature_rows = truncated_coefficients(jnp.dot(standardized_entries, attribute_projection, preferred_element_type=jnp.float32)).reshape(-1, ATTENDER_TOTAL, DH)
        coefficient_array = partition_share_entries(standardized_entries, assignment_feeder_projection, partition_projection, partition_offset, softmax_sharpness)
        coefficients_halfprecision = truncated_coefficients(coefficient_array)
        return ((running_state[0] + lax.optimization_barrier(jnp.sum(coefficient_array, axis=0)), running_state[1] + jnp.einsum('qct,qcv->ctv', coefficients_halfprecision, slice_feature_rows)), None)
    start = (jnp.zeros((ATTENDER_TOTAL, M), jnp.float32), jnp.zeros((ATTENDER_TOTAL, M, DH), jnp.float32))
    (totals, numerator), unused = lax.scan(gather_sums, start, row_blocks)
    slice_token = numerator / (totals + 1e-05)[:, :, None]
    highest_mode = lax.Precision.HIGHEST
    query_rows = jnp.einsum('izn,nu->izu', slice_token, partition_question_map, precision=highest_mode)
    key_vectors = jnp.einsum('izn,nu->izu', slice_token, partition_lookup_map, precision=highest_mode)
    value_rows = jnp.einsum('izn,nu->izu', slice_token, partition_content_map, precision=highest_mode)
    score_scale = 1.0 / math.sqrt(DH)
    scores = jnp.einsum('hme,hne->hmn', query_rows, key_vectors, precision=highest_mode) * score_scale
    attention = jax.nn.softmax(scores, axis=-1)
    slice_output = truncated_coefficients(jnp.einsum('hmn,hne->hme', attention, value_rows, precision=highest_mode))
    inverse = jnp.argsort(inference_placement).astype(jnp.int32).reshape(block_count, PTS_DEV)

    def serve_block(serve_index):
        row_block = jnp.take(layer_inputs_trainorder, serve_index, axis=0)
        standardized_entries = layer_norm(row_block.astype(jnp.float32), initial_layernorm_gain, initial_layernorm_offset).astype(jnp.bfloat16)
        coefficients_halfprecision = truncated_coefficients(partition_share_entries(standardized_entries, assignment_feeder_projection, partition_projection, partition_offset, softmax_sharpness))
        blended_rows = jnp.einsum('fny,nyp->fnp', coefficients_halfprecision, slice_output).astype(jnp.bfloat16).reshape(-1, MODEL_CHANNELS)
        hidden = row_block.astype(jnp.float32) + jnp.dot(blended_rows, emitted_projection, preferred_element_type=jnp.float32) + emitted_offset
        normed_two = layer_norm(hidden, latter_layernorm_gain, latter_layernorm_offset).astype(jnp.bfloat16)
        inner_act = jax.nn.gelu(jnp.dot(normed_two, perceptron_entry_map, preferred_element_type=jnp.float32) + perceptron_entry_offset, approximate=False).astype(jnp.bfloat16)
        return (hidden + jnp.dot(inner_act, perceptron_exit_map, preferred_element_type=jnp.float32) + perceptron_exit_offset).astype(jnp.bfloat16)
    served = lax.map(serve_block, inverse)
    return served.reshape(N_PTS, SERVE, MODEL_CHANNELS)
```

```python
import functools
import math

import jax
import jax.numpy as jnp
from jax import lax
from jax.experimental import pallas as pl
from jax.experimental.pallas import tpu as pltpu
from jax.sharding import PartitionSpec as P

MESH = pl.DeviceIdType.MESH
BF = jnp.bfloat16
F32 = jnp.float32
DEVS = 128
ROWS = 6144
PER = 48
C = 256
HEADS, DH, M = 16, 16, 32
SL = HEADS * M
LOG2E = math.log2(math.e)
HI = lax.Precision.HIGHEST
BLK = 256
BLK2 = 384


def iota(shape, dim):
    return lax.broadcasted_iota(jnp.int32, shape, dim)


def nt(a, b, **kw):
    return lax.dot_general(a, b, (((1,), (1,)), ((), ())), preferred_element_type=F32, **kw)


def tn(a, b, **kw):
    return lax.dot_general(a, b, (((0,), (0,)), ((), ())), preferred_element_type=F32, **kw)


def nn(a, b, **kw):
    return jnp.dot(a, b, preferred_element_type=F32, **kw)


def layer_norm(x, gain, bias):
    mean = jnp.mean(x, axis=-1, keepdims=True)
    c = x - mean
    var = jnp.mean(c * c, axis=-1, keepdims=True)
    return c * lax.rsqrt(var + 1e-05) * gain + bias


def slice_m(shape, dim):
    return (iota(shape, dim) % 256) // 8


def slice_h(shape, dim):
    r = iota(shape, dim)
    return (r // 256) * 8 + r % 8


def head_mask():
    return slice_h((SL, C), 0) == iota((SL, C), 1) // DH


def wide_partition(part):
    cols = (iota((DH, C), 1) % DH == iota((DH, C), 0)).astype(BF)
    z = tn(part, cols).astype(BF)
    pick = (slice_m((SL, M), 0) == iota((SL, M), 1)).astype(BF)
    return jnp.where(head_mask(), nn(pick, z), 0.0).astype(BF)


def offset_rows(off):
    pick = (iota((256, M), 0) // 8 == iota((256, M), 1)).astype(F32)
    return nt(pick, jnp.broadcast_to(off, (128, M)), precision=HI)


def slice_softmax(logit_ref, off_ref, inv_ref, width, emit):
    for hh in range(2):
        inv = inv_ref[hh * 8 : hh * 8 + 8, :]
        for lb in range(width // 128):
            a = logit_ref[hh * 256 : hh * 256 + 256, lb * 128 : lb * 128 + 128]
            a = (a + off_ref[...]).reshape(M, 8, 128) * inv
            e = jnp.exp2(a - jnp.max(a, axis=0))
            sw = e * (1.0 / jnp.sum(e, axis=0))
            emit(hh, lb, sw.reshape(256, 128))


def order_kernel(x_ref, pos_ref, xs_ref, lbl_ref, src, dst, ord_v, ord_s, sem):
    def widen(i, _):
        blk = x_ref[pl.ds(i * 16, 16), :].astype(F32)
        src[pl.ds(i * 32, 16, stride=2), :] = blk[:, :128]
        src[pl.ds(i * 32 + 1, 16, stride=2), :] = blk[:, 128:]
        return 0

    lax.fori_loop(0, ROWS // 16, widen, 0, unroll=4)

    before = (iota((256, 256), 0) < iota((256, 256), 1)).astype(BF)
    tri = jnp.concatenate([before, jnp.ones((256, 128), BF)], axis=1)

    def block(k, carry):
        count, acc = carry
        pos = jnp.concatenate([pos_ref[2 * k], pos_ref[2 * k + 1]], axis=1)
        blk = ((pos >> 11) * 21846) >> 16
        inside = pos - blk * ROWS
        target = (blk & 7) * 16 + (blk >> 3)
        me = k * 256 + iota((1, 256), 1)
        hot = (iota((DEVS, 256), 0) == target).astype(F32)
        hot_b = hot.astype(BF)
        ahead = nn(hot_b, tri)
        full = ahead[:, :256] + jnp.concatenate([count, count], axis=1)
        rank = jnp.sum(hot * full, axis=0, keepdims=True).astype(jnp.int32)
        same = iota((64, 256), 0) == rank
        parts = [inside >> 6, inside & 63, me >> 6, me & 63]
        vals = [jnp.where(same, v.astype(F32), 0.0) for v in parts]
        acc = acc + nt(hot_b, jnp.concatenate(vals, axis=0).astype(BF))
        return count + ahead[:, 256:], acc

    zero = jnp.zeros((DEVS, 128), F32)
    _, acc = lax.fori_loop(
        0, ROWS // 256, block, (zero, jnp.zeros((DEVS, 256), F32)), unroll=4
    )
    acc = acc.astype(jnp.int32)
    label = acc[:, 0:64] * 64 + acc[:, 64:128]
    order = acc[:, 128:192] * 64 + acc[:, 192:256]
    pad = jnp.zeros((DEVS, 64), jnp.int32)
    lbl_ref[...] = jnp.concatenate([label, pad], axis=1).reshape(DEVS, 1, 128)
    ord_v[...] = jnp.concatenate([order, pad], axis=1)
    copy = pltpu.make_async_copy(ord_v, ord_s, sem)
    copy.start()
    copy.wait()

    def gather(t, _):
        for r in range(PER):
            dst[pl.ds(t * 96 + 2 * r, 2), :] = src[pl.ds(ord_s[t, r] * 2, 2), :]
        for q in range(PER // 16):
            left = dst[pl.ds(t * 96 + q * 32, 16, stride=2), :]
            right = dst[pl.ds(t * 96 + q * 32 + 1, 16, stride=2), :]
            xs_ref[pl.ds(t * PER + q * 16, 16), :] = jnp.concatenate(
                [left, right], axis=1
            ).astype(BF)
        return 0

    lax.fori_loop(0, DEVS, gather, 0)


def exchange_kernel(
    xs, lbl, sharp, g1, b1, w_f, w_x, part, off, wq, wk, wv,
    rows_in, lbl_in, sout_ref, inv_ref,
    logit, swt, fx_s, acc, tot, bigp, offs, pay, rs, hd, mine, res, shp,
    row_send, row_recv, lbl_send, lbl_recv, small_send, small_recv, own_sem,
):
    h = lax.axis_index("head")
    p = lax.axis_index("pts")
    me = h * 16 + p
    z0, y0, x0, c0 = h // 2, (p // 8) * 2 + h % 2, (p // 2) % 4, p % 2

    def partner(k):
        k = (k * 53) % 128
        z = (z0 + k // 32) % 4
        y = (y0 + (k // 8) % 4) % 4
        x = (x0 + (k // 2) % 4) % 4
        c = (c0 + k % 2) % 2
        return z * 2 + y % 2, (y // 2) * 8 + x * 2 + c

    bar = pltpu.get_barrier_semaphore()

    def greet(k, _):
        pl.semaphore_signal(bar, inc=1, device_id=partner(k), device_id_type=MESH)
        return 0

    lax.fori_loop(1, DEVS, greet, 0)

    own_rows = pltpu.make_async_copy(xs.at[me], rows_in.at[me], own_sem.at[0])
    own_lbl = pltpu.make_async_copy(lbl.at[me], lbl_in.at[me], own_sem.at[1])
    own_rows.start()
    own_lbl.start()
    bigp[...] = wide_partition(part[...])
    offs[...] = offset_rows(off[...])
    acc[...] = jnp.zeros_like(acc)
    tot[...] = jnp.zeros_like(tot)
    pl.semaphore_wait(bar, DEVS - 1)

    def send_small(src, dst, dev, i):
        return pltpu.make_async_remote_copy(
            src_ref=src, dst_ref=dst, send_sem=small_send.at[i], recv_sem=small_recv.at[i],
            device_id=dev, device_id_type=MESH,
        )

    def send_rows(k, _):
        dev = partner(k)
        to = dev[0] * 16 + dev[1]
        pltpu.make_async_remote_copy(
            src_ref=xs.at[to], dst_ref=rows_in.at[me], send_sem=row_send, recv_sem=row_recv,
            device_id=dev, device_id_type=MESH,
        ).start()
        pltpu.make_async_remote_copy(
            src_ref=lbl.at[to], dst_ref=lbl_in.at[me], send_sem=lbl_send, recv_sem=lbl_recv,
            device_id=dev, device_id_type=MESH,
        ).start()
        return 0

    temps = [
        send_small(sharp, shp.at[h], ((h + i) % 8, p), i - 1) for i in range(1, 8)
    ]
    for t in temps:
        t.start()
    shp[h] = sharp[...]
    lax.fori_loop(1, 9, send_rows, 0)
    for t in temps:
        t.wait()
    inv_ref[...] = LOG2E / jnp.concatenate([shp[i] for i in range(8)], axis=0)

    def pass_one(i, _):
        send_rows(9 + i, 0)
        x = xs_flat(xs, i)
        normed = layer_norm(x.astype(F32), g1[...], b1[...]).astype(BF)
        fx_s[...] = nn(normed, w_f[...]).astype(BF)
        xm = nn(normed, w_x[...]).astype(BF)
        logit[...] = nt(bigp[...], xm)

        def emit(hh, lb, sw):
            tot[hh * 256 : hh * 256 + 256, :] += sw
            swt[hh * 256 : hh * 256 + 256, lb * 128 : lb * 128 + 128] = sw.astype(BF)

        slice_softmax(logit, offs, inv_ref, 384, emit)
        acc[...] += nn(swt[...], fx_s[...])
        return 0

    lax.fori_loop(0, ROWS // 384, pass_one, 0)

    mask = head_mask()

    def fold(a):
        a = jnp.where(mask, a, 0.0)
        return jnp.sum(a[:256].reshape(M, 8, C) + a[256:].reshape(M, 8, C), axis=1)

    numer = fold(acc[...])
    total = fold(jnp.broadcast_to(jnp.sum(tot[...], axis=1, keepdims=True), (SL, C)))
    for i, a in enumerate((numer, total)):
        for rg in range(4):
            for lt in range(2):
                pay[i * 8 + rg * 2 + lt] = a[rg * 8 : rg * 8 + 8, lt * 128 : lt * 128 + 128]
    first = [
        send_small(pay.at[(p + i) % 16], rs.at[p], (h, (p + i) % 16), 6 + i)
        for i in range(1, 16)
    ]
    for t in first:
        t.start()
    rs[p] = pay[p]
    lax.fori_loop(25, 35, send_rows, 0)
    for t in first:
        t.wait()
    mine[...] = jnp.sum(rs[...], axis=0)
    second = [send_small(mine, hd.at[h], ((h + i) % 8, p), 21 + i) for i in range(1, 8)]
    for t in second:
        t.start()
    hd[h] = mine[...]
    lax.fori_loop(35, 45, send_rows, 0)
    for t in second:
        t.wait()
    pay[0] = jnp.sum(hd[...], axis=0)
    third = [
        send_small(pay.at[0], res.at[p], (h, (p + i) % 16), 28 + i) for i in range(1, 16)
    ]
    for t in third:
        t.start()
    res[p] = pay[0]
    lax.fori_loop(45, DEVS, send_rows, 0)
    for t in third:
        t.wait()

    def gathered(i):
        return jnp.concatenate(
            [
                jnp.concatenate([res[i * 8 + rg * 2], res[i * 8 + rg * 2 + 1]], axis=1)
                for rg in range(4)
            ],
            axis=0,
        )

    stok = gathered(0) / (gathered(1) + 1e-05)
    same_head = iota((C, C), 0) // DH == iota((C, C), 1) // DH
    rep = (iota((C, DH), 0) % DH == iota((C, DH), 1)).astype(F32)

    def per_head(w):
        wide = nt(nn(rep, w[...], precision=HI), rep, precision=HI)
        return jnp.where(same_head, wide, 0.0)

    q = nn(stok, per_head(wq), precision=HI)
    k = nn(stok, per_head(wk), precision=HI)
    v = nn(stok, per_head(wv), precision=HI)

    def spread(a):
        a = jnp.broadcast_to(a[:, None, :], (M, 8, C)).reshape(256, C)
        return jnp.where(mask, jnp.concatenate([a, a], axis=0), 0.0)

    score = nt(spread(k), q, precision=HI) * (1.0 / math.sqrt(DH))
    score = score.reshape(2, M, 8, M)
    e = jnp.exp(score - jnp.max(score, axis=1, keepdims=True))
    att = (e / jnp.sum(e, axis=1, keepdims=True)).reshape(SL, M)
    sout = tn(att, spread(v), precision=HI)
    sout_ref[...] = spread(sout).astype(BF)

    own_rows.wait()
    own_lbl.wait()
    n = DEVS - 1
    nbr = partner(1)
    pltpu.make_async_remote_copy(
        src_ref=xs.at[pl.ds(0, n)], dst_ref=rows_in.at[pl.ds(0, n)], send_sem=row_send,
        recv_sem=row_recv, device_id=nbr, device_id_type=MESH,
    ).wait()
    pltpu.make_async_remote_copy(
        src_ref=lbl.at[pl.ds(0, n)], dst_ref=lbl_in.at[pl.ds(0, n)], send_sem=lbl_send,
        recv_sem=lbl_recv, device_id=nbr, device_id_type=MESH,
    ).wait()


def xs_flat(xs, i):
    return xs[pl.ds(i * 8, 8)].reshape(384, C)


def serve_kernel(
    x_ref, lbl_ref, sout_ref, inv_ref, g1, b1, w_x, part, off, w_e, b_e, g2, b2, w_1, b_1,
    w_2, b_2, out_ref, logit, swt, bigp, offs, stage, flat,
):
    bigp[...] = wide_partition(part[...])
    offs[...] = offset_rows(off[...])

    def pass_two(i, _):
        x = x_ref[pl.ds(i * BLK2, BLK2), :].astype(F32)
        normed = layer_norm(x, g1[...], b1[...]).astype(BF)
        xm = nn(normed, w_x[...]).astype(BF)
        logit[...] = nt(bigp[...], xm)

        def emit(hh, lb, sw):
            swt[hh * 256 : hh * 256 + 256, lb * 128 : lb * 128 + 128] = sw.astype(BF)

        slice_softmax(logit, offs, inv_ref, BLK2, emit)
        o = tn(swt[...], sout_ref[...]).astype(BF)
        y = x + nn(o, w_e[...]) + b_e[...]
        z = layer_norm(y, g2[...], b2[...]).astype(BF)
        u = nn(z, w_1[...]) + b_1[...]
        g = (0.5 * u * (1.0 + lax.erf(u * math.sqrt(0.5)))).astype(BF)
        y = y + nn(g, w_2[...]) + b_2[...]
        stage[pl.ds(0, BLK2, stride=2), :] = y[:, :128]
        stage[pl.ds(1, BLK2, stride=2), :] = y[:, 128:]
        for s in range(BLK2 // PER):
            for r in range(PER):
                flat[pl.ds(lbl_ref[i * 8 + s, r] * 2, 2), :] = stage[
                    pl.ds((s * PER + r) * 2, 2), :
                ]
        return 0

    lax.fori_loop(0, ROWS // BLK2, pass_two, 0)

    def narrow(i, _):
        left = flat[pl.ds(i * 32, 16, stride=2), :]
        right = flat[pl.ds(i * 32 + 1, 16, stride=2), :]
        out_ref[pl.ds(i * 16, 16), :] = jnp.concatenate([left, right], axis=1).astype(BF)
        return 0

    lax.fori_loop(0, ROWS // 16, narrow, 0, unroll=4)


VM = pl.BlockSpec(memory_space=pltpu.VMEM)
SM = pl.BlockSpec(memory_space=pltpu.SMEM)
LIMIT = 60 * 1024 * 1024


def order_rows(x, pos):
    return pl.pallas_call(
        order_kernel,
        out_shape=[
            jax.ShapeDtypeStruct((ROWS, C), BF),
            jax.ShapeDtypeStruct((DEVS, 1, 128), jnp.int32),
        ],
        in_specs=[VM] * 2,
        out_specs=[VM] * 2,
        scratch_shapes=[
            pltpu.VMEM((ROWS * 2, 128), F32),
            pltpu.VMEM((ROWS * 2, 128), F32),
            pltpu.VMEM((DEVS, 128), jnp.int32),
            pltpu.SMEM((DEVS, 128), jnp.int32),
            pltpu.SemaphoreType.DMA,
        ],
        compiler_params=pltpu.CompilerParams(vmem_limit_bytes=LIMIT),
        name="order_rows",
    )(x, pos)


def exchange(*args):
    dma = pltpu.SemaphoreType.DMA
    return pl.pallas_call(
        exchange_kernel,
        out_shape=[
            jax.ShapeDtypeStruct((DEVS, PER, C), BF),
            jax.ShapeDtypeStruct((DEVS, 1, 128), jnp.int32),
            jax.ShapeDtypeStruct((SL, C), BF),
            jax.ShapeDtypeStruct((HEADS, 128), F32),
        ],
        in_specs=[VM] * len(args),
        out_specs=[VM] * 4,
        scratch_shapes=[
            pltpu.VMEM((SL, 384), F32),
            pltpu.VMEM((SL, 384), BF),
            pltpu.VMEM((384, C), BF),
            pltpu.VMEM((SL, C), F32),
            pltpu.VMEM((SL, 128), F32),
            pltpu.VMEM((SL, C), BF),
            pltpu.VMEM((256, 128), F32),
            pltpu.VMEM((16, 8, 128), F32),
            pltpu.VMEM((16, 8, 128), F32),
            pltpu.VMEM((8, 8, 128), F32),
            pltpu.VMEM((8, 128), F32),
            pltpu.VMEM((16, 8, 128), F32),
            pltpu.VMEM((8, 2, 128), F32),
            dma, dma, dma, dma, dma((44,)), dma((44,)), dma((2,)),
        ],
        compiler_params=pltpu.CompilerParams(
            vmem_limit_bytes=LIMIT, collective_id=0, has_side_effects=True
        ),
        name="exchange",
    )(*args)


def serve_rows(*args):
    return pl.pallas_call(
        serve_kernel,
        out_shape=jax.ShapeDtypeStruct((ROWS, C), BF),
        in_specs=[VM, SM] + [VM] * (len(args) - 2),
        out_specs=VM,
        scratch_shapes=[
            pltpu.VMEM((SL, BLK2), F32),
            pltpu.VMEM((SL, BLK2), BF),
            pltpu.VMEM((SL, C), BF),
            pltpu.VMEM((256, 128), F32),
            pltpu.VMEM((BLK2 * 2, 128), F32),
            pltpu.VMEM((ROWS * 2, 128), F32),
        ],
        compiler_params=pltpu.CompilerParams(vmem_limit_bytes=LIMIT),
        name="serve_rows",
    )(*args)


def body(
    x, pos, g1, b1, w_f, w_x, part, off, sharp, wq, wk, wv, w_e, b_e, g2, b2, w_1, b_1, w_2, b_2
):
    row = lambda a: a.reshape(1, -1)
    xs, lbl = order_rows(x, pos.reshape(48, 1, 128))
    sharp = jnp.broadcast_to(sharp[:, None], (2, 128))
    rows_in, lbl_in, sout, inv = exchange(
        xs.reshape(DEVS, PER, C), lbl, sharp, row(g1), row(b1), w_f, w_x, part, row(off),
        wq, wk, wv,
    )
    served = serve_rows(
        rows_in.reshape(ROWS, C), lbl_in.reshape(DEVS, 128), sout, inv, row(g1), row(b1), w_x,
        part, row(off), w_e, row(b_e), row(g2), row(b2), w_1, row(b_1), w_2, row(b_2),
    )
    return served[None]


def solution(mesh):
    both = ("head", "pts")
    in_specs = (P(both, None), P(both)) + (P(),) * 6 + (P("head"),) + (P(),) * 11
    return jax.shard_map(
        body, mesh=mesh, in_specs=in_specs, out_specs=P("pts", "head", None), check_vma=False
    )
```

```python
import functools
import math

import jax
import jax.numpy as jnp
from jax import lax
from jax.experimental import pallas as pl
from jax.experimental.pallas import tpu as pltpu
from jax.sharding import PartitionSpec as P

MESH = pl.DeviceIdType.MESH
BF = jnp.bfloat16
F32 = jnp.float32
DEVS = 128
ROWS = 6144
PER = 48
C = 256
HEADS, DH, M = 16, 16, 32
SL = HEADS * M
LOG2E = math.log2(math.e)
HI = lax.Precision.HIGHEST
BLK = 768


def iota(shape, dim):
    return lax.broadcasted_iota(jnp.int32, shape, dim)


def nt(a, b, **kw):
    return lax.dot_general(a, b, (((1,), (1,)), ((), ())), preferred_element_type=F32, **kw)


def tn(a, b, **kw):
    return lax.dot_general(a, b, (((0,), (0,)), ((), ())), preferred_element_type=F32, **kw)


def nn(a, b, **kw):
    return jnp.dot(a, b, preferred_element_type=F32, **kw)


def layer_norm(x, gain, bias):
    mean = jnp.mean(x, axis=-1, keepdims=True)
    c = x - mean
    var = jnp.mean(c * c, axis=-1, keepdims=True)
    return c * lax.rsqrt(var + 1e-05) * gain + bias


def slice_m(shape, dim):
    return (iota(shape, dim) % 256) // 8


def slice_h(shape, dim):
    r = iota(shape, dim)
    return (r // 256) * 8 + r % 8


def head_mask():
    return slice_h((SL, C), 0) == iota((SL, C), 1) // DH


def wide_partition(part):
    cols = (iota((DH, C), 1) % DH == iota((DH, C), 0)).astype(BF)
    z = tn(part, cols).astype(BF)
    pick = (slice_m((SL, M), 0) == iota((SL, M), 1)).astype(BF)
    return jnp.where(head_mask(), nn(pick, z), 0.0).astype(BF)


def offset_rows(off):
    pick = (iota((256, M), 0) // 8 == iota((256, M), 1)).astype(F32)
    return nt(pick, jnp.broadcast_to(off, (128, M)), precision=HI)


def slice_softmax(logit_ref, off_ref, inv_ref, width, emit):
    for hh in range(2):
        inv = inv_ref[hh * 8 : hh * 8 + 8, :]
        for lb in range(width // 128):
            a = logit_ref[hh * 256 : hh * 256 + 256, lb * 128 : lb * 128 + 128]
            a = (a + off_ref[...]).reshape(M, 8, 128) * inv
            e = jnp.exp2(a - jnp.max(a, axis=0))
            sw = e * (1.0 / jnp.sum(e, axis=0))
            emit(hh, lb, sw.reshape(256, 128))


def exchange_kernel(
    x_hbm, pos_ref, sharp, g1, b1, w_f, w_x, part, off, wq, wk, wv, w_e, b_e, g2, b2, w_1, b_1,
    w_2, b_2, y_hbm, lbl_in,
    xv, src, hop, xsend, rows_in, lbl, ord_v, ord_s, logit, swt, fx_s, acc, tot, bigp, offs,
    wide, pay, rs, hd, mine, res, shp, inv_ref, sout_ref, stage,
    x_sem, ord_sem, y_sem, row_send, row_recv, lbl_send, lbl_recv, small_send, small_recv,
):
    h = lax.axis_index("head")
    p = lax.axis_index("pts")
    z0, y0, x0, c0 = h // 2, (p // 8) * 2 + h % 2, (p // 2) % 4, p % 2

    def partner(k):
        k = (k * 53) % 128
        z = (z0 + k // 32) % 4
        y = (y0 + (k // 8) % 4) % 4
        x = (x0 + (k // 2) % 4) % 4
        c = (c0 + k % 2) % 2
        return z * 2 + y % 2, (y // 2) * 8 + x * 2 + c

    load_x = pltpu.make_async_copy(x_hbm, xv, x_sem)
    load_x.start()
    bar = pltpu.get_barrier_semaphore()

    def greet(k, _):
        pl.semaphore_signal(bar, inc=1, device_id=partner(k), device_id_type=MESH)
        return 0

    lax.fori_loop(1, DEVS, greet, 0)

    before = (iota((256, 256), 0) < iota((256, 256), 1)).astype(BF)
    tri = jnp.concatenate([before, jnp.ones((256, 128), BF)], axis=1)

    def block(k, carry):
        count, total = carry
        pos = jnp.concatenate([pos_ref[2 * k], pos_ref[2 * k + 1]], axis=1)
        blk = ((pos >> 11) * 21846) >> 16
        inside = pos - blk * ROWS
        target = (blk & 7) * 16 + (blk >> 3)
        me = k * 256 + iota((1, 256), 1)
        hot = (iota((DEVS, 256), 0) == target).astype(F32)
        hot_b = hot.astype(BF)
        ahead = nn(hot_b, tri)
        full = ahead[:, :256] + jnp.concatenate([count, count], axis=1)
        rank = jnp.sum(hot * full, axis=0, keepdims=True).astype(jnp.int32)
        same = iota((64, 256), 0) == rank
        parts = [inside >> 6, inside & 63, me >> 6, me & 63]
        vals = [jnp.where(same, v.astype(F32), 0.0) for v in parts]
        total = total + nt(hot_b, jnp.concatenate(vals, axis=0).astype(BF))
        return count + ahead[:, 256:], total

    zero = jnp.zeros((DEVS, 128), F32)
    _, order = lax.fori_loop(
        0, ROWS // 256, block, (zero, jnp.zeros((DEVS, 256), F32)), unroll=4
    )
    order = order.astype(jnp.int32)
    pad = jnp.zeros((DEVS, 64), jnp.int32)
    label = order[:, 0:64] * 64 + order[:, 64:128]
    lbl[...] = jnp.concatenate([label * 2, pad], axis=1).reshape(DEVS, 1, 128)
    order = order[:, 128:192] * 64 + order[:, 192:256]
    order = jnp.clip(order * 2, 0, ROWS * 2 - 2)
    ord_v[...] = jnp.concatenate([order, pad], axis=1)
    save_order = pltpu.make_async_copy(ord_v, ord_s, ord_sem)
    save_order.start()
    load_x.wait()

    def widen(i, _):
        blk = xv[pl.ds(i * 16, 16), :].astype(F32)
        src[pl.ds(i * 32, 16, stride=2), :] = blk[:, :128]
        src[pl.ds(i * 32 + 1, 16, stride=2), :] = blk[:, 128:]
        return 0

    lax.fori_loop(0, ROWS // 16, widen, 0, unroll=8)
    save_order.wait()

    def gather(k, _):
        dev = partner(k)
        to = dev[0] * 16 + dev[1]
        for r in range(PER):
            hop[2 * r : 2 * r + 2, :] = src[pl.ds(ord_s[to, r], 2), :]
        for q in range(PER // 16):
            left = hop[pl.ds(q * 32, 16, stride=2), :]
            right = hop[pl.ds(q * 32 + 1, 16, stride=2), :]
            both = jnp.concatenate([left, right], axis=1).astype(BF)
            xsend[k, q * 16 : q * 16 + 16, :] = both
        return 0

    lax.fori_loop(0, 9, gather, 0)
    rows_in[0] = xsend[0]
    lbl_in[0] = lbl[h * 16 + p]

    bigp[...] = wide_partition(part[...])
    offs[...] = offset_rows(off[...])
    same_head = iota((C, C), 0) // DH == iota((C, C), 1) // DH
    rep = (iota((C, DH), 0) % DH == iota((C, DH), 1)).astype(F32)
    for i, w in enumerate((wq, wk, wv)):
        full = nt(nn(rep, w[...], precision=HI), rep, precision=HI)
        wide[i] = jnp.where(same_head, full, 0.0)
    acc[...] = jnp.zeros_like(acc)
    tot[...] = jnp.zeros_like(tot)
    pl.semaphore_wait(bar, DEVS - 1)

    def send_small(src, dst, dev, i):
        return pltpu.make_async_remote_copy(
            src_ref=src, dst_ref=dst, send_sem=small_send.at[i], recv_sem=small_recv.at[i],
            device_id=dev, device_id_type=MESH,
        )

    def send_rows(k, _):
        dev = partner(k)
        to = dev[0] * 16 + dev[1]
        pltpu.make_async_remote_copy(
            src_ref=xsend.at[k], dst_ref=rows_in.at[k], send_sem=row_send,
            recv_sem=row_recv.at[k // 16], device_id=dev, device_id_type=MESH,
        ).start()
        pltpu.make_async_remote_copy(
            src_ref=lbl.at[to], dst_ref=lbl_in.at[k], send_sem=lbl_send, recv_sem=lbl_recv,
            device_id=dev, device_id_type=MESH,
        ).start()
        return 0

    def move(first, count, ahead):
        lax.fori_loop(first, first + count, send_rows, 0)
        lax.fori_loop(first + count, first + count + ahead, gather, 0)

    temps = [send_small(sharp, shp.at[h], ((h + i) % 8, p), i - 1) for i in range(1, 8)]
    for t in temps:
        t.start()
    shp[h] = sharp[...]
    move(1, 8, 6)
    for t in temps:
        t.wait()
    inv_ref[...] = LOG2E / jnp.concatenate([shp[i] for i in range(8)], axis=0)

    def pass_one(i, _):
        move(9 + 6 * i, 6, 6)
        normed = layer_norm(xv[pl.ds(i * BLK, BLK), :].astype(F32), g1[...], b1[...]).astype(BF)
        fx_s[...] = nn(normed, w_f[...]).astype(BF)
        xm = nn(normed, w_x[...]).astype(BF)
        logit[...] = nt(bigp[...], xm)

        def emit(hh, lb, sw):
            tot[hh * 256 : hh * 256 + 256, :] += sw
            swt[hh * 256 : hh * 256 + 256, lb * 128 : lb * 128 + 128] = sw.astype(BF)

        slice_softmax(logit, offs, inv_ref, BLK, emit)
        acc[...] += nn(swt[...], fx_s[...])
        return 0

    lax.fori_loop(0, ROWS // BLK, pass_one, 0)

    mask = head_mask()

    def fold(a):
        a = jnp.where(mask, a, 0.0)
        return jnp.sum(a[:256].reshape(M, 8, C) + a[256:].reshape(M, 8, C), axis=1)

    numer = fold(acc[...])
    total = fold(jnp.broadcast_to(jnp.sum(tot[...], axis=1, keepdims=True), (SL, C)))
    for i, a in enumerate((numer, total)):
        for rg in range(4):
            for lt in range(2):
                pay[i * 8 + rg * 2 + lt] = a[rg * 8 : rg * 8 + 8, lt * 128 : lt * 128 + 128]
    first = [
        send_small(pay.at[(p + i) % 16], rs.at[p], (h, (p + i) % 16), 6 + i)
        for i in range(1, 16)
    ]
    for t in first:
        t.start()
    rs[p] = pay[p]
    move(57, 6, 10)
    for t in first:
        t.wait()
    mine[...] = jnp.sum(rs[...], axis=0)
    second = [send_small(mine, hd.at[h], ((h + i) % 8, p), 21 + i) for i in range(1, 8)]
    for t in second:
        t.start()
    hd[h] = mine[...]
    move(63, 10, 10)
    for t in second:
        t.wait()
    pay[0] = jnp.sum(hd[...], axis=0)
    third = [
        send_small(pay.at[0], res.at[p], (h, (p + i) % 16), 28 + i) for i in range(1, 16)
    ]
    for t in third:
        t.start()
    res[p] = pay[0]
    move(73, 10, 45)
    lax.fori_loop(83, DEVS, send_rows, 0)
    for t in third:
        t.wait()

    def gathered(i):
        return jnp.concatenate(
            [
                jnp.concatenate([res[i * 8 + rg * 2], res[i * 8 + rg * 2 + 1]], axis=1)
                for rg in range(4)
            ],
            axis=0,
        )

    stok = gathered(0) / (gathered(1) + 1e-05)
    q, k, v = (nn(stok, wide[i], precision=HI) for i in range(3))

    def spread(a):
        a = jnp.broadcast_to(a[:, None, :], (M, 8, C)).reshape(256, C)
        return jnp.where(mask, jnp.concatenate([a, a], axis=0), 0.0)

    score = nt(spread(k), q, precision=HI) * (1.0 / math.sqrt(DH))
    score = score.reshape(2, M, 8, M)
    e = jnp.exp(score - jnp.max(score, axis=1, keepdims=True))
    att = (e / jnp.sum(e, axis=1, keepdims=True)).reshape(SL, M)
    sout = tn(att, spread(v), precision=HI)
    sout_ref[...] = spread(sout).astype(BF)

    nbr = partner(1)

    def arrived(n, sem):
        pltpu.make_async_remote_copy(
            src_ref=xsend.at[pl.ds(0, n)], dst_ref=rows_in.at[pl.ds(0, n)], send_sem=row_send,
            recv_sem=sem, device_id=nbr, device_id_type=MESH,
        ).wait_recv()

    def pass_two(i, _):
        @pl.when(i == 0)
        def _():
            arrived(15, row_recv.at[0])

        @pl.when(i > 0)
        def _():
            arrived(16, row_recv.at[i])

        x = rows_in[pl.ds(i * 16, 16)].reshape(BLK, C).astype(F32)
        normed = layer_norm(x, g1[...], b1[...]).astype(BF)
        xm = nn(normed, w_x[...]).astype(BF)
        logit[...] = nt(bigp[...], xm)

        def emit(hh, lb, sw):
            swt[hh * 256 : hh * 256 + 256, lb * 128 : lb * 128 + 128] = sw.astype(BF)

        slice_softmax(logit, offs, inv_ref, BLK, emit)
        o = tn(swt[...], sout_ref[...]).astype(BF)
        y = x + nn(o, w_e[...]) + b_e[...]
        z = layer_norm(y, g2[...], b2[...]).astype(BF)
        u = nn(z, w_1[...]) + b_1[...]
        g = (u * (1.0 + lax.erf(u * math.sqrt(0.5)))).astype(BF)
        y = y + 0.5 * nn(g, w_2[...]) + b_2[...]
        at = i * BLK * 2
        stage[pl.ds(at, BLK, stride=2), :] = y[:, :128]
        stage[pl.ds(at + 1, BLK, stride=2), :] = y[:, 128:]
        rows = pl.ds(at, BLK * 2)
        pltpu.make_async_copy(stage.at[rows], y_hbm.at[rows], y_sem.at[i]).start()
        return 0

    lax.fori_loop(0, ROWS // BLK, pass_two, 0)

    n = DEVS - 1
    pltpu.make_async_remote_copy(
        src_ref=xsend.at[pl.ds(0, n)], dst_ref=rows_in.at[pl.ds(0, n)], send_sem=row_send,
        recv_sem=row_recv.at[0], device_id=nbr, device_id_type=MESH,
    ).wait_send()
    pltpu.make_async_remote_copy(
        src_ref=lbl.at[pl.ds(0, n)], dst_ref=lbl_in.at[pl.ds(0, n)], send_sem=lbl_send,
        recv_sem=lbl_recv, device_id=nbr, device_id_type=MESH,
    ).wait()
    for i in range(ROWS // BLK):
        rows = pl.ds(i * BLK * 2, BLK * 2)
        pltpu.make_async_copy(stage.at[rows], y_hbm.at[rows], y_sem.at[i]).wait()


PIECES = 8


def place_kernel(y_hbm, lbl_ref, out_hbm, y, flat, out_v, in_sem, out_sem):
    size = ROWS * 2 // PIECES
    loads = []
    for i in range(PIECES):
        rows = pl.ds(i * size, size)
        loads.append(pltpu.make_async_copy(y_hbm.at[rows], y.at[rows], in_sem.at[i]))
        loads[-1].start()

    def scatter(t, _):
        for r in range(PER):
            flat[pl.ds(lbl_ref[t, r], 2), :] = y[pl.ds(t * PER * 2 + 2 * r, 2), :]
        return 0

    for i in range(PIECES):
        loads[i].wait()
        lax.fori_loop(i * DEVS // PIECES, (i + 1) * DEVS // PIECES, scatter, 0, unroll=2)

    def narrow(i, _):
        left = flat[pl.ds(i * 32, 16, stride=2), :]
        right = flat[pl.ds(i * 32 + 1, 16, stride=2), :]
        out_v[pl.ds(i * 16, 16), :] = jnp.concatenate([left, right], axis=1).astype(BF)
        return 0

    stores = []
    for i in range(PIECES):
        lo, hi = i * ROWS // PIECES, (i + 1) * ROWS // PIECES
        lax.fori_loop(lo // 16, hi // 16, narrow, 0, unroll=8)
        rows = pl.ds(lo, hi - lo)
        stores.append(pltpu.make_async_copy(out_v.at[rows], out_hbm.at[rows], out_sem.at[i]))
        stores[-1].start()
    for s in stores:
        s.wait()


VM = pl.BlockSpec(memory_space=pltpu.VMEM)
SM = pl.BlockSpec(memory_space=pltpu.SMEM)
ANY = pl.BlockSpec(memory_space=pl.ANY)
LIMIT = 60 * 1024 * 1024


def exchange(*args):
    dma = pltpu.SemaphoreType.DMA
    return pl.pallas_call(
        exchange_kernel,
        out_shape=[
            jax.ShapeDtypeStruct((ROWS * 2, 128), F32),
            jax.ShapeDtypeStruct((DEVS, 1, 128), jnp.int32),
        ],
        in_specs=[ANY] + [VM] * (len(args) - 1),
        out_specs=[ANY, VM],
        scratch_shapes=[
            pltpu.VMEM((ROWS, C), BF),
            pltpu.VMEM((ROWS * 2, 128), F32),
            pltpu.VMEM((PER * 2, 128), F32),
            pltpu.VMEM((DEVS, PER, C), BF),
            pltpu.VMEM((DEVS, PER, C), BF),
            pltpu.VMEM((DEVS, 1, 128), jnp.int32),
            pltpu.VMEM((DEVS, 128), jnp.int32),
            pltpu.SMEM((DEVS, 128), jnp.int32),
            pltpu.VMEM((SL, BLK), F32),
            pltpu.VMEM((SL, BLK), BF),
            pltpu.VMEM((BLK, C), BF),
            pltpu.VMEM((SL, C), F32),
            pltpu.VMEM((SL, 128), F32),
            pltpu.VMEM((SL, C), BF),
            pltpu.VMEM((256, 128), F32),
            pltpu.VMEM((3, C, C), F32),
            pltpu.VMEM((16, 8, 128), F32),
            pltpu.VMEM((16, 8, 128), F32),
            pltpu.VMEM((8, 8, 128), F32),
            pltpu.VMEM((8, 128), F32),
            pltpu.VMEM((16, 8, 128), F32),
            pltpu.VMEM((8, 2, 128), F32),
            pltpu.VMEM((HEADS, 128), F32),
            pltpu.VMEM((SL, C), BF),
            pltpu.VMEM((ROWS * 2, 128), F32),
            dma, dma, dma((ROWS // BLK,)), dma, dma((8,)), dma, dma, dma((44,)), dma((44,)),
        ],
        compiler_params=pltpu.CompilerParams(
            vmem_limit_bytes=LIMIT, collective_id=0, has_side_effects=True
        ),
        name="exchange",
    )(*args)


def place_rows(y, lbl):
    return pl.pallas_call(
        place_kernel,
        out_shape=jax.ShapeDtypeStruct((ROWS, C), BF),
        in_specs=[ANY, SM],
        out_specs=ANY,
        scratch_shapes=[
            pltpu.VMEM((ROWS * 2, 128), F32),
            pltpu.VMEM((ROWS * 2, 128), F32),
            pltpu.VMEM((ROWS, C), BF),
            pltpu.SemaphoreType.DMA((PIECES,)),
            pltpu.SemaphoreType.DMA((PIECES,)),
        ],
        compiler_params=pltpu.CompilerParams(vmem_limit_bytes=LIMIT),
        name="place_rows",
    )(y, lbl)


def body(
    x, pos, g1, b1, w_f, w_x, part, off, sharp, wq, wk, wv, w_e, b_e, g2, b2, w_1, b_1, w_2, b_2
):
    row = lambda a: a.reshape(1, -1)
    y, lbl = exchange(
        x, pos.reshape(48, 1, 128), jnp.broadcast_to(sharp[:, None], (2, 128)), row(g1),
        row(b1), w_f, w_x, part, row(off), wq, wk, wv, w_e, row(b_e), row(g2), row(b2), w_1,
        row(b_1), w_2, row(b_2),
    )
    return place_rows(y, lbl.reshape(DEVS, 128))[None]


def solution(mesh):
    both = ("head", "pts")
    in_specs = (P(both, None), P(both)) + (P(),) * 6 + (P("head"),) + (P(),) * 11
    return jax.shard_map(
        body, mesh=mesh, in_specs=in_specs, out_specs=P("pts", "head", None), check_vma=False
    )
```

```python
import functools
import math

import jax
import jax.numpy as jnp
from jax import lax
from jax.experimental import pallas as pl
from jax.experimental.pallas import tpu as pltpu
from jax.sharding import PartitionSpec as P

MESH = pl.DeviceIdType.MESH
BF = jnp.bfloat16
F32 = jnp.float32
DEVS = 128
ROWS = 6144
PER = 48
C = 256
HEADS, DH, M = 16, 16, 32
SL = HEADS * M
LOG2E = math.log2(math.e)
HI = lax.Precision.HIGHEST
BLK = 768
SUB = 256
FSUB = 384
EARLY = 6


def iota(shape, dim):
    return lax.broadcasted_iota(jnp.int32, shape, dim)


def nt(a, b, **kw):
    return lax.dot_general(a, b, (((1,), (1,)), ((), ())), preferred_element_type=F32, **kw)


def tn(a, b, **kw):
    return lax.dot_general(a, b, (((0,), (0,)), ((), ())), preferred_element_type=F32, **kw)


def nn(a, b, **kw):
    return jnp.dot(a, b, preferred_element_type=F32, **kw)


def layer_norm(x, gain, bias):
    mean = jnp.mean(x, axis=-1, keepdims=True)
    c = x - mean
    var = jnp.mean(c * c, axis=-1, keepdims=True)
    return c * lax.rsqrt(var + 1e-05) * gain + bias


def slice_m(shape, dim):
    return (iota(shape, dim) % 256) // 8


def slice_h(shape, dim):
    r = iota(shape, dim)
    return (r // 256) * 8 + r % 8


def head_mask():
    return slice_h((SL, C), 0) == iota((SL, C), 1) // DH


def wide_partition(part):
    cols = (iota((DH, C), 1) % DH == iota((DH, C), 0)).astype(BF)
    z = tn(part, cols).astype(BF)
    pick = (slice_m((SL, M), 0) == iota((SL, M), 1)).astype(BF)
    return jnp.where(head_mask(), nn(pick, z), 0.0).astype(BF)


def offset_rows(off):
    pick = (iota((256, M), 0) // 8 == iota((256, M), 1)).astype(F32)
    return nt(pick, jnp.broadcast_to(off, (128, M)), precision=HI)


def skewed(count, *stages):
    for step in range(count + len(stages) - 1):
        for t in reversed(range(len(stages))):
            if 0 <= step - t < count:
                stages[t](step - t)


def slice_softmax(logit_ref, off_ref, inv_ref, lanes, emit):
    for hh in range(2):
        inv = inv_ref[hh * 8 : hh * 8 + 8, :]
        for lb in lanes:
            a = logit_ref[hh * 256 : hh * 256 + 256, lb * 128 : lb * 128 + 128]
            a = (a + off_ref[...]).reshape(M, 8, 128) * inv
            e = jnp.exp2(a - jnp.max(a, axis=0))
            sw = e * (1.0 / jnp.sum(e, axis=0))
            emit(hh, lb, sw.reshape(256, 128))


def sub_lanes(s):
    return range(s * SUB // 128, (s + 1) * SUB // 128)


def exchange_kernel(
    x_hbm, pos_ref, sharp, g1, b1, w_f, w_x, part, off, wq, wk, wv, w_e, b_e, g2, b2, w_1, b_1,
    w_2, b_2, y_hbm, lbl_in,
    xv, src, hop, xsend, rows_in, lbl, ord_v, ord_s, logit, swt, fx_s, acc, tot, bigp, offs,
    wide, pay, rs, hd, mine, res, own_temp, shp, inv_ref, sout_ref, stage,
    x_sem, ord_sem, y_sem, row_send, row_recv, lbl_send, lbl_recv, small_send, small_recv,
):
    h = lax.axis_index("head")
    p = lax.axis_index("pts")
    z0, y0, x0, c0 = h >> 1, ((p >> 3) << 1) + (h & 1), (p >> 1) & 3, p & 1

    def partner(k):
        k = (k * 53) & 127
        z = (z0 + (k >> 5)) & 3
        y = (y0 + (k >> 3)) & 3
        x = (x0 + (k >> 1)) & 3
        c = (c0 + k) & 1
        return z * 2 + (y & 1), (y >> 1) * 8 + x * 2 + c

    load_x = pltpu.make_async_copy(x_hbm, xv, x_sem)
    load_x.start()
    both = [jnp.full((1, 128), sharp[i], F32) for i in range(2)]
    own_temp[...] = jnp.concatenate(both, axis=0)
    bar = pltpu.get_barrier_semaphore()

    def greet(k, _):
        pl.semaphore_signal(bar, inc=1, device_id=partner(k), device_id_type=MESH)
        return 0

    lax.fori_loop(1, DEVS, greet, 0, unroll=4)

    before = (iota((256, 256), 0) < iota((256, 256), 1)).astype(BF)
    tri = jnp.concatenate([before, jnp.ones((256, 128), BF)], axis=1)

    def block(k, carry):
        count, total = carry
        pos = jnp.concatenate([pos_ref[2 * k], pos_ref[2 * k + 1]], axis=1)
        blk = ((pos >> 11) * 21846) >> 16
        inside = pos - blk * ROWS
        target = (blk & 7) * 16 + (blk >> 3)
        me = k * 256 + iota((1, 256), 1)
        hot = (iota((DEVS, 256), 0) == target).astype(F32)
        hot_b = hot.astype(BF)
        ahead = nn(hot_b, tri)
        full = ahead[:, :256] + jnp.concatenate([count, count], axis=1)
        rank = jnp.sum(hot * full, axis=0, keepdims=True).astype(jnp.int32)
        same = iota((64, 256), 0) == rank
        parts = [inside >> 6, inside & 63, me >> 6, me & 63]
        vals = [jnp.where(same, v.astype(F32), 0.0) for v in parts]
        total = total + nt(hot_b, jnp.concatenate(vals, axis=0).astype(BF))
        return count + ahead[:, 256:], total

    zero = jnp.zeros((DEVS, 128), F32)
    _, order = lax.fori_loop(
        0, ROWS // 256, block, (zero, jnp.zeros((DEVS, 256), F32)), unroll=4
    )
    order = order.astype(jnp.int32)
    pad = jnp.zeros((DEVS, 64), jnp.int32)
    label = order[:, 0:64] * 64 + order[:, 64:128]
    lbl[...] = jnp.concatenate([label * 2, pad], axis=1).reshape(DEVS, 1, 128)
    order = order[:, 128:192] * 64 + order[:, 192:256]
    order = jnp.clip(order * 2, 0, ROWS * 2 - 2)
    ord_v[...] = jnp.concatenate([order, pad], axis=1)
    save_order = pltpu.make_async_copy(ord_v, ord_s, ord_sem)
    save_order.start()
    pl.semaphore_wait(bar, DEVS - 1)

    def send_small(src, dst, dev, i):
        return pltpu.make_async_remote_copy(
            src_ref=src, dst_ref=dst, send_sem=small_send.at[i], recv_sem=small_recv.at[i],
            device_id=dev, device_id_type=MESH,
        )

    def send_rows(k, _):
        dev = partner(k)
        to = dev[0] * 16 + dev[1]
        pltpu.make_async_remote_copy(
            src_ref=xsend.at[k], dst_ref=rows_in.at[k], send_sem=row_send,
            recv_sem=row_recv.at[k // 16], device_id=dev, device_id_type=MESH,
        ).start()
        pltpu.make_async_remote_copy(
            src_ref=lbl.at[to], dst_ref=lbl_in.at[k], send_sem=lbl_send, recv_sem=lbl_recv,
            device_id=dev, device_id_type=MESH,
        ).start()
        return 0

    def send(first, stop):
        lax.fori_loop(first, stop, send_rows, 0)

    shp[h] = own_temp[...]
    temps = [send_small(own_temp, shp.at[h], ((h + i) % 8, p), i - 1) for i in range(1, 8)]
    for t in temps:
        t.start()
    load_x.wait()

    def widen(i, _):
        blk = xv[pl.ds(i * 16, 16), :].astype(F32)
        src[pl.ds(i * 32, 16, stride=2), :] = blk[:, :128]
        src[pl.ds(i * 32 + 1, 16, stride=2), :] = blk[:, 128:]
        return 0

    lax.fori_loop(0, ROWS // 16, widen, 0, unroll=8)
    save_order.wait()

    def gather(first, count):
        for i in range(count):
            dev = partner(first + i)
            picks = ord_s.at[dev[0] * 16 + dev[1]]
            for r in range(PER):
                at = (i * PER + r) * 2
                hop[at : at + 2, :] = src[pl.ds(picks[r], 2), :]
            for q in range(PER // 16):
                at = i * PER * 2 + q * 32
                left = hop[pl.ds(at, 16, stride=2), :]
                right = hop[pl.ds(at + 1, 16, stride=2), :]
                both = jnp.concatenate([left, right], axis=1).astype(BF)
                xsend[first + i, q * 16 : q * 16 + 16, :] = both

    gather(0, 16)
    rows_in[0] = xsend[0]
    lbl_in[0] = lbl[h * 16 + p]

    send(1, 7)
    bigp[...] = wide_partition(part[...])
    offs[...] = offset_rows(off[...])
    same_head = iota((C, C), 0) // DH == iota((C, C), 1) // DH
    rep = (iota((C, DH), 0) % DH == iota((C, DH), 1)).astype(F32)
    for i, w in enumerate((wq, wk, wv)):
        full = nt(nn(rep, w[...], precision=HI), rep, precision=HI)
        wide[i] = jnp.where(same_head, full, 0.0)
    acc[...] = jnp.zeros_like(acc)
    tot[...] = jnp.zeros_like(tot)
    for t in temps:
        t.wait()
    inv_ref[...] = LOG2E / jnp.concatenate([shp[i] for i in range(8)], axis=0)

    def pass_one(i, _):
        send(7 + 9 * i, 16 + 9 * i)
        gather(16 + 14 * i, 14)
        normed, xm = {}, {}

        def norm(s):
            x = xv[pl.ds(i * BLK + s * SUB, SUB), :].astype(F32)
            normed[s] = layer_norm(x, g1[...], b1[...]).astype(BF)

        def project(s):
            fx_s[s * SUB : s * SUB + SUB, :] = nn(normed[s], w_f[...]).astype(BF)
            xm[s] = nn(normed[s], w_x[...]).astype(BF)

        def score(s):
            logit[:, s * SUB : s * SUB + SUB] = nt(bigp[...], xm[s])

        def weights(s):
            def emit(hh, lb, sw):
                tot[hh * 256 : hh * 256 + 256, :] += sw
                swt[0, hh * 256 : hh * 256 + 256, lb * 128 : lb * 128 + 128] = sw.astype(BF)

            slice_softmax(logit, offs, inv_ref, sub_lanes(s), emit)

        skewed(BLK // SUB, norm, project, score, weights)
        acc[...] += nn(swt[0], fx_s[...])
        return 0

    lax.fori_loop(0, ROWS // BLK, pass_one, 0)

    nbr = partner(1)

    def arrived(n, sem):
        pltpu.make_async_remote_copy(
            src_ref=xsend.at[pl.ds(0, n)], dst_ref=rows_in.at[pl.ds(0, n)], send_sem=row_send,
            recv_sem=sem, device_id=nbr, device_id_type=MESH,
        ).wait_recv()

    def weigh(i):
        normed, xm = {}, {}

        def norm(s):
            x = rows_in[pl.ds(i * 16, 16)].reshape(BLK, C)[s * SUB : s * SUB + SUB].astype(F32)
            normed[s] = layer_norm(x, g1[...], b1[...]).astype(BF)

        def project(s):
            xm[s] = nn(normed[s], w_x[...]).astype(BF)

        def score(s):
            logit[:, s * SUB : s * SUB + SUB] = nt(bigp[...], xm[s])

        def weights(s):
            def emit(hh, lb, sw):
                swt[i, hh * 256 : hh * 256 + 256, lb * 128 : lb * 128 + 128] = sw.astype(BF)

            slice_softmax(logit, offs, inv_ref, sub_lanes(s), emit)

        skewed(BLK // SUB, norm, project, score, weights)

    def weigh_sending(first, count):
        def step(i, _):
            send(first + count * i, first + count + count * i)

            @pl.when(i == 0)
            def _():
                arrived(15, row_recv.at[0])

            @pl.when(i > 0)
            def _():
                arrived(16, row_recv.at[i])

            weigh(i)
            return 0

        return step

    mask = head_mask()

    def fold(a):
        a = jnp.where(mask, a, 0.0)
        return jnp.sum(a[:256].reshape(M, 8, C) + a[256:].reshape(M, 8, C), axis=1)

    numer = fold(acc[...])
    total = fold(jnp.broadcast_to(jnp.sum(tot[...], axis=1, keepdims=True), (SL, C)))
    for i, a in enumerate((numer, total)):
        for rg in range(4):
            for lt in range(2):
                pay[i * 8 + rg * 2 + lt] = a[rg * 8 : rg * 8 + 8, lt * 128 : lt * 128 + 128]
    first = [
        send_small(pay.at[(p + i) % 16], rs.at[p], (h, (p + i) % 16), 6 + i)
        for i in range(1, 16)
    ]
    for t in first:
        t.start()
    rs[p] = pay[p]
    step = weigh_sending(79, 4)
    lax.fori_loop(0, 2, step, 0)
    for t in first:
        t.wait()
    mine[...] = jnp.sum(rs[...], axis=0)
    second = [send_small(mine, hd.at[h], ((h + i) % 8, p), 21 + i) for i in range(1, 8)]
    for t in second:
        t.start()
    hd[h] = mine[...]
    lax.fori_loop(2, 4, step, 0)
    for t in second:
        t.wait()
    pay[0] = jnp.sum(hd[...], axis=0)
    third = [
        send_small(pay.at[0], res.at[p], (h, (p + i) % 16), 28 + i) for i in range(1, 16)
    ]
    for t in third:
        t.start()
    res[p] = pay[0]
    send(79 + 4 * 4, DEVS)
    lax.fori_loop(4, EARLY, weigh_sending(0, 0), 0)
    for t in third:
        t.wait()

    def gathered(i):
        return jnp.concatenate(
            [
                jnp.concatenate([res[i * 8 + rg * 2], res[i * 8 + rg * 2 + 1]], axis=1)
                for rg in range(4)
            ],
            axis=0,
        )

    stok = gathered(0) / (gathered(1) + 1e-05)
    q, k, v = (nn(stok, wide[i], precision=HI) for i in range(3))

    def spread(a):
        a = jnp.broadcast_to(a[:, None, :], (M, 8, C)).reshape(256, C)
        return jnp.where(mask, jnp.concatenate([a, a], axis=0), 0.0)

    score = nt(spread(k), q, precision=HI) * (1.0 / math.sqrt(DH))
    score = score.reshape(2, M, 8, M)
    e = jnp.exp(score - jnp.max(score, axis=1, keepdims=True))
    att = (e / jnp.sum(e, axis=1, keepdims=True)).reshape(SL, M)
    sout = tn(att, spread(v), precision=HI)
    sout_ref[...] = spread(sout).astype(BF)

    def finish(i):
        o, y, z, g = {}, {}, {}, {}

        def blend(s):
            o[s] = tn(swt[i, :, s * FSUB : s * FSUB + FSUB], sout_ref[...]).astype(BF)

        def norm(s):
            x = rows_in[pl.ds(i * 16, 16)].reshape(BLK, C)[s * FSUB : s * FSUB + FSUB]
            y[s] = x.astype(F32) + nn(o[s], w_e[...]) + b_e[...]
            z[s] = layer_norm(y[s], g2[...], b2[...]).astype(BF)

        def enter(s):
            u = nn(z[s], w_1[...]) + b_1[...]
            g[s] = (u * (1.0 + lax.erf(u * math.sqrt(0.5)))).astype(BF)

        def leave(s):
            a = y[s] + 0.5 * nn(g[s], w_2[...]) + b_2[...]
            at = i * BLK * 2 + s * FSUB * 2
            stage[pl.ds(at, FSUB, stride=2), :] = a[:, :128]
            stage[pl.ds(at + 1, FSUB, stride=2), :] = a[:, 128:]

        skewed(BLK // FSUB, blend, norm, enter, leave)
        rows = pl.ds(i * BLK * 2, BLK * 2)
        pltpu.make_async_copy(stage.at[rows], y_hbm.at[rows], y_sem.at[i]).start()

    def finish_early(i, _):
        finish(i)
        return 0

    def finish_late(i, _):
        arrived(16, row_recv.at[i])
        weigh(i)
        finish(i)
        return 0

    lax.fori_loop(0, EARLY, finish_early, 0)
    lax.fori_loop(EARLY, ROWS // BLK, finish_late, 0)

    n = DEVS - 1
    pltpu.make_async_remote_copy(
        src_ref=xsend.at[pl.ds(0, n)], dst_ref=rows_in.at[pl.ds(0, n)], send_sem=row_send,
        recv_sem=row_recv.at[0], device_id=nbr, device_id_type=MESH,
    ).wait_send()
    pltpu.make_async_remote_copy(
        src_ref=lbl.at[pl.ds(0, n)], dst_ref=lbl_in.at[pl.ds(0, n)], send_sem=lbl_send,
        recv_sem=lbl_recv, device_id=nbr, device_id_type=MESH,
    ).wait()
    for i in range(ROWS // BLK):
        rows = pl.ds(i * BLK * 2, BLK * 2)
        pltpu.make_async_copy(stage.at[rows], y_hbm.at[rows], y_sem.at[i]).wait()


PIECES = 8


def place_kernel(y_hbm, lbl_ref, out_hbm, y, flat, out_v, in_sem, out_sem):
    size = ROWS * 2 // PIECES
    loads = []
    for i in range(PIECES):
        rows = pl.ds(i * size, size)
        loads.append(pltpu.make_async_copy(y_hbm.at[rows], y.at[rows], in_sem.at[i]))
        loads[-1].start()

    def scatter(t, _):
        places = lbl_ref.at[t]
        for r in range(PER):
            flat[pl.ds(places[r], 2), :] = y[pl.ds(t * PER * 2 + 2 * r, 2), :]
        return 0

    for i in range(PIECES):
        loads[i].wait()
        lax.fori_loop(i * DEVS // PIECES, (i + 1) * DEVS // PIECES, scatter, 0, unroll=2)

    def narrow(i, _):
        left = flat[pl.ds(i * 32, 16, stride=2), :]
        right = flat[pl.ds(i * 32 + 1, 16, stride=2), :]
        out_v[pl.ds(i * 16, 16), :] = jnp.concatenate([left, right], axis=1).astype(BF)
        return 0

    stores = []
    for i in range(PIECES):
        lo, hi = i * ROWS // PIECES, (i + 1) * ROWS // PIECES
        lax.fori_loop(lo // 16, hi // 16, narrow, 0, unroll=8)
        rows = pl.ds(lo, hi - lo)
        stores.append(pltpu.make_async_copy(out_v.at[rows], out_hbm.at[rows], out_sem.at[i]))
        stores[-1].start()
    for s in stores:
        s.wait()


VM = pl.BlockSpec(memory_space=pltpu.VMEM)
SM = pl.BlockSpec(memory_space=pltpu.SMEM)
ANY = pl.BlockSpec(memory_space=pl.ANY)
LIMIT = 60 * 1024 * 1024


def exchange(*args):
    dma = pltpu.SemaphoreType.DMA
    return pl.pallas_call(
        exchange_kernel,
        out_shape=[
            jax.ShapeDtypeStruct((ROWS * 2, 128), F32),
            jax.ShapeDtypeStruct((DEVS, 1, 128), jnp.int32),
        ],
        in_specs=[ANY, VM, SM] + [VM] * (len(args) - 3),
        out_specs=[ANY, VM],
        scratch_shapes=[
            pltpu.VMEM((ROWS, C), BF),
            pltpu.VMEM((ROWS * 2, 128), F32),
            pltpu.VMEM((16 * PER * 2, 128), F32),
            pltpu.VMEM((DEVS, PER, C), BF),
            pltpu.VMEM((DEVS, PER, C), BF),
            pltpu.VMEM((DEVS, 1, 128), jnp.int32),
            pltpu.VMEM((DEVS, 128), jnp.int32),
            pltpu.SMEM((DEVS, 128), jnp.int32),
            pltpu.VMEM((SL, BLK), F32),
            pltpu.VMEM((ROWS // BLK, SL, BLK), BF),
            pltpu.VMEM((BLK, C), BF),
            pltpu.VMEM((SL, C), F32),
            pltpu.VMEM((SL, 128), F32),
            pltpu.VMEM((SL, C), BF),
            pltpu.VMEM((256, 128), F32),
            pltpu.VMEM((3, C, C), F32),
            pltpu.VMEM((16, 8, 128), F32),
            pltpu.VMEM((16, 8, 128), F32),
            pltpu.VMEM((8, 8, 128), F32),
            pltpu.VMEM((8, 128), F32),
            pltpu.VMEM((16, 8, 128), F32),
            pltpu.VMEM((2, 128), F32),
            pltpu.VMEM((8, 2, 128), F32),
            pltpu.VMEM((HEADS, 128), F32),
            pltpu.VMEM((SL, C), BF),
            pltpu.VMEM((ROWS * 2, 128), F32),
            dma, dma, dma((ROWS // BLK,)), dma, dma((8,)), dma, dma, dma((44,)), dma((44,)),
        ],
        compiler_params=pltpu.CompilerParams(
            vmem_limit_bytes=LIMIT, collective_id=0, has_side_effects=True
        ),
        name="exchange",
    )(*args)


def place_rows(y, lbl):
    return pl.pallas_call(
        place_kernel,
        out_shape=jax.ShapeDtypeStruct((ROWS, C), BF),
        in_specs=[ANY, SM],
        out_specs=ANY,
        scratch_shapes=[
            pltpu.VMEM((ROWS * 2, 128), F32),
            pltpu.VMEM((ROWS * 2, 128), F32),
            pltpu.VMEM((ROWS, C), BF),
            pltpu.SemaphoreType.DMA((PIECES,)),
            pltpu.SemaphoreType.DMA((PIECES,)),
        ],
        compiler_params=pltpu.CompilerParams(vmem_limit_bytes=LIMIT),
        name="place_rows",
    )(y, lbl)


def body(
    x, pos, g1, b1, w_f, w_x, part, off, sharp, wq, wk, wv, w_e, b_e, g2, b2, w_1, b_1, w_2, b_2
):
    row = lambda a: a.reshape(1, -1)
    y, lbl = exchange(
        x, pos.reshape(48, 1, 128), sharp, row(g1),
        row(b1), w_f, w_x, part, row(off), wq, wk, wv, w_e, row(b_e), row(g2), row(b2), w_1,
        row(b_1), w_2, row(b_2),
    )
    return place_rows(y, lbl.reshape(DEVS, 128))[None]


def solution(mesh):
    both = ("head", "pts")
    in_specs = (P(both, None), P(both)) + (P(),) * 6 + (P("head"),) + (P(),) * 11
    return jax.shard_map(
        body, mesh=mesh, in_specs=in_specs, out_specs=P("pts", "head", None), check_vma=False
    )
```

```python
import functools
import math

import jax
import jax.numpy as jnp
from jax import lax
from jax.experimental import pallas as pl
from jax.experimental.pallas import tpu as pltpu
from jax.sharding import PartitionSpec as P

MESH = pl.DeviceIdType.MESH
BF = jnp.bfloat16
F32 = jnp.float32
DEVS = 128
ROWS = 6144
PER = 48
C = 256
HEADS, DH, M = 16, 16, 32
SL = HEADS * M
LOG2E = math.log2(math.e)
HI = lax.Precision.HIGHEST
BLK = 768
SUB = 256
FSUB = 384
EARLY = 4


def iota(shape, dim):
    return lax.broadcasted_iota(jnp.int32, shape, dim)


def nt(a, b, **kw):
    return lax.dot_general(a, b, (((1,), (1,)), ((), ())), preferred_element_type=F32, **kw)


def tn(a, b, **kw):
    return lax.dot_general(a, b, (((0,), (0,)), ((), ())), preferred_element_type=F32, **kw)


def nn(a, b, **kw):
    return jnp.dot(a, b, preferred_element_type=F32, **kw)


def layer_norm(x, gain, bias):
    mean = jnp.mean(x, axis=-1, keepdims=True)
    c = x - mean
    var = jnp.mean(c * c, axis=-1, keepdims=True)
    return c * lax.rsqrt(var + 1e-05) * gain + bias


def slice_m(shape, dim):
    return (iota(shape, dim) % 256) // 8


def slice_h(shape, dim):
    r = iota(shape, dim)
    return (r // 256) * 8 + r % 8


def head_mask():
    return slice_h((SL, C), 0) == iota((SL, C), 1) // DH


def wide_partition(part):
    cols = (iota((DH, C), 1) % DH == iota((DH, C), 0)).astype(BF)
    z = tn(part, cols).astype(BF)
    pick = (slice_m((SL, M), 0) == iota((SL, M), 1)).astype(BF)
    return jnp.where(head_mask(), nn(pick, z), 0.0).astype(BF)


def offset_rows(off):
    pick = (iota((256, M), 0) // 8 == iota((256, M), 1)).astype(F32)
    return nt(pick, jnp.broadcast_to(off, (128, M)), precision=HI)


def skewed(count, *stages):
    for step in range(count + len(stages) - 1):
        for t in reversed(range(len(stages))):
            if 0 <= step - t < count:
                stages[t](step - t)


def slice_softmax(logit_ref, off_ref, inv_ref, lanes, emit):
    for hh in range(2):
        inv = inv_ref[hh * 8 : hh * 8 + 8, :]
        for lb in lanes:
            a = logit_ref[hh * 256 : hh * 256 + 256, lb * 128 : lb * 128 + 128]
            a = (a + off_ref[...]).reshape(M, 8, 128) * inv
            e = jnp.exp2(a - jnp.max(a, axis=0))
            sw = e * (1.0 / jnp.sum(e, axis=0))
            emit(hh, lb, sw.reshape(256, 128))


def sub_lanes(s):
    return range(s * SUB // 128, (s + 1) * SUB // 128)


def exchange_kernel(
    x_hbm, pos_ref, sharp, g1, b1, w_f, w_x, part, off, wq, wk, wv, w_e, b_e, g2, b2, w_1, b_1,
    w_2, b_2, y_hbm, lbl_in,
    xv, src, hop, xsend, rows_in, lbl, ord_v, ord_s, logit, swt, swr, fx_s, acc, tot, bigp, offs,
    wide, pay, rs, hd, mine, res, own_temp, shp, inv_ref, sout_ref, stage,
    x_sem, ord_sem, y_sem, row_send, row_recv, lbl_send, lbl_recv, small_send, small_recv,
):
    h = lax.axis_index("head")
    p = lax.axis_index("pts")
    z0, y0, x0, c0 = h >> 1, ((p >> 3) << 1) + (h & 1), (p >> 1) & 3, p & 1

    at_z = [((z0 + i) & 3) * 2 for i in range(4)]
    at_y = [(y0 + i) & 3 for i in range(4)]
    at_y = [(y & 1, (y >> 1) * 8) for y in at_y]
    at_x = [((x0 + i) & 3) * 2 for i in range(4)]
    at_c = [(c0 + i) & 1 for i in range(2)]

    def partner(k):
        if isinstance(k, int):
            k = (k * 53) & 127
            y = at_y[(k >> 3) & 3]
            return at_z[k >> 5] + y[0], y[1] + at_x[(k >> 1) & 3] + at_c[k & 1]
        k = (k * 53) & 127
        z = (z0 + (k >> 5)) & 3
        y = (y0 + (k >> 3)) & 3
        x = (x0 + (k >> 1)) & 3
        c = (c0 + k) & 1
        return z * 2 + (y & 1), (y >> 1) * 8 + x * 2 + c

    load_x = pltpu.make_async_copy(x_hbm, xv, x_sem)
    load_x.start()
    both = [jnp.full((1, 128), sharp[i], F32) for i in range(2)]
    own_temp[...] = jnp.concatenate(both, axis=0)
    bar = pltpu.get_barrier_semaphore()

    for k in range(1, DEVS):
        pl.semaphore_signal(bar, inc=1, device_id=partner(k), device_id_type=MESH)

    before = (iota((256, 256), 0) < iota((256, 256), 1)).astype(BF)
    tri = jnp.concatenate([before, jnp.ones((256, 128), BF)], axis=1)

    def block(k, carry):
        count, total = carry
        pos = jnp.concatenate([pos_ref[2 * k], pos_ref[2 * k + 1]], axis=1)
        blk = ((pos >> 11) * 21846) >> 16
        inside = pos - blk * ROWS
        target = (blk & 7) * 16 + (blk >> 3)
        me = k * 256 + iota((1, 256), 1)
        hot = (iota((DEVS, 256), 0) == target).astype(F32)
        hot_b = hot.astype(BF)
        ahead = nn(hot_b, tri)
        full = ahead[:, :256] + jnp.concatenate([count, count], axis=1)
        rank = jnp.sum(hot * full, axis=0, keepdims=True).astype(jnp.int32)
        same = iota((64, 256), 0) == rank
        parts = [inside >> 6, inside & 63, me >> 6, me & 63]
        vals = [jnp.where(same, v.astype(F32), 0.0) for v in parts]
        total = total + nt(hot_b, jnp.concatenate(vals, axis=0).astype(BF))
        return count + ahead[:, 256:], total

    zero = jnp.zeros((DEVS, 128), F32)
    _, order = lax.fori_loop(
        0, ROWS // 256, block, (zero, jnp.zeros((DEVS, 256), F32)), unroll=4
    )
    order = order.astype(jnp.int32)
    pad = jnp.zeros((DEVS, 64), jnp.int32)
    label = order[:, 0:64] * 64 + order[:, 64:128]
    lbl[...] = jnp.concatenate([label * 2, pad], axis=1).reshape(DEVS, 1, 128)
    order = order[:, 128:192] * 64 + order[:, 192:256]
    order = jnp.clip(order * 2, 0, ROWS * 2 - 2)
    ord_v[...] = jnp.concatenate([order, pad], axis=1)
    save_order = pltpu.make_async_copy(ord_v, ord_s, ord_sem)
    save_order.start()
    pl.semaphore_wait(bar, DEVS - 1)

    def send_small(src, dst, dev, i):
        return pltpu.make_async_remote_copy(
            src_ref=src, dst_ref=dst, send_sem=small_send.at[i], recv_sem=small_recv.at[i],
            device_id=dev, device_id_type=MESH,
        )

    def send_rows(k):
        dev = partner(k)
        to = dev[0] * 16 + dev[1]
        pltpu.make_async_remote_copy(
            src_ref=xsend.at[k], dst_ref=rows_in.at[k], send_sem=row_send,
            recv_sem=row_recv.at[k // 16], device_id=dev, device_id_type=MESH,
        ).start()
        pltpu.make_async_remote_copy(
            src_ref=lbl.at[to], dst_ref=lbl_in.at[k], send_sem=lbl_send, recv_sem=lbl_recv,
            device_id=dev, device_id_type=MESH,
        ).start()

    def send(first, count):
        for k in range(count):
            send_rows(first + k)

    shp[h] = own_temp[...]
    temps = [send_small(own_temp, shp.at[h], ((h + i) % 8, p), i - 1) for i in range(1, 8)]
    for t in temps:
        t.start()
    load_x.wait()

    def widen(i, _):
        blk = xv[pl.ds(i * 16, 16), :].astype(F32)
        src[pl.ds(i * 32, 16, stride=2), :] = blk[:, :128]
        src[pl.ds(i * 32 + 1, 16, stride=2), :] = blk[:, 128:]
        return 0

    lax.fori_loop(0, ROWS // 16, widen, 0, unroll=8)
    save_order.wait()

    def gather(first, count):
        for i in range(count):
            dev = partner(first + i)
            picks = ord_s.at[dev[0] * 16 + dev[1]]
            for r in range(PER):
                at = (i * PER + r) * 2
                hop[at : at + 2, :] = src[pl.ds(picks[r], 2), :]
            for q in range(PER // 16):
                at = i * PER * 2 + q * 32
                left = hop[pl.ds(at, 16, stride=2), :]
                right = hop[pl.ds(at + 1, 16, stride=2), :]
                both = jnp.concatenate([left, right], axis=1).astype(BF)
                xsend[first + i, q * 16 : q * 16 + 16, :] = both

    gather(0, 16)
    rows_in[0] = xsend[0]
    lbl_in[0] = lbl[h * 16 + p]

    send(1, 6)
    bigp[...] = wide_partition(part[...])
    offs[...] = offset_rows(off[...])
    same_head = iota((C, C), 0) // DH == iota((C, C), 1) // DH
    rep = (iota((C, DH), 0) % DH == iota((C, DH), 1)).astype(F32)
    for i, w in enumerate((wq, wk, wv)):
        full = nt(nn(rep, w[...], precision=HI), rep, precision=HI)
        wide[i] = jnp.where(same_head, full, 0.0)
    acc[...] = jnp.zeros_like(acc)
    tot[...] = jnp.zeros_like(tot)
    for t in temps:
        t.wait()
    inv_ref[...] = LOG2E / jnp.concatenate([shp[i] for i in range(8)], axis=0)

    def pass_one(i, _):
        send(7 + 7 * i, 7)
        gather(16 + 14 * i, 14)
        normed, xm = {}, {}

        def norm(s):
            x = xv[pl.ds(i * BLK + s * SUB, SUB), :].astype(F32)
            normed[s] = layer_norm(x, g1[...], b1[...]).astype(BF)

        def project(s):
            fx_s[s * SUB : s * SUB + SUB, :] = nn(normed[s], w_f[...]).astype(BF)
            xm[s] = nn(normed[s], w_x[...]).astype(BF)

        def score(s):
            logit[:, s * SUB : s * SUB + SUB] = nt(bigp[...], xm[s])

        def weights(s):
            def emit(hh, lb, sw):
                tot[hh * 256 : hh * 256 + 256, :] += sw
                swt[hh * 256 : hh * 256 + 256, lb * 128 : lb * 128 + 128] = sw.astype(BF)

            slice_softmax(logit, offs, inv_ref, sub_lanes(s), emit)

        skewed(BLK // SUB, norm, project, score, weights)
        acc[...] += nn(swt[...], fx_s[...])
        return 0

    lax.fori_loop(0, ROWS // BLK, pass_one, 0)

    nbr = partner(1)

    def arrived(n, sem):
        pltpu.make_async_remote_copy(
            src_ref=xsend.at[pl.ds(0, n)], dst_ref=rows_in.at[pl.ds(0, n)], send_sem=row_send,
            recv_sem=sem, device_id=nbr, device_id_type=MESH,
        ).wait_recv()

    def weigh(i):
        normed, xm = {}, {}

        def norm(s):
            x = rows_in[pl.ds(i * 16, 16)].reshape(BLK, C)[s * SUB : s * SUB + SUB].astype(F32)
            normed[s] = layer_norm(x, g1[...], b1[...]).astype(BF)

        def project(s):
            xm[s] = nn(normed[s], w_x[...]).astype(BF)

        def score(s):
            logit[:, s * SUB : s * SUB + SUB] = nt(bigp[...], xm[s])

        def weights(s):
            def emit(hh, lb, sw):
                swr[i, lb * 128 : lb * 128 + 128, hh * 256 : hh * 256 + 256] = sw.astype(BF).T

            slice_softmax(logit, offs, inv_ref, sub_lanes(s), emit)

        skewed(BLK // SUB, norm, project, score, weights)

    def weigh_sending(first, count):
        def step(i, _):
            send(first + count * i, count)

            @pl.when(i == 0)
            def _():
                arrived(15, row_recv.at[0])

            @pl.when(i > 0)
            def _():
                arrived(16, row_recv.at[i])

            weigh(i)
            return 0

        return step

    mask = head_mask()

    def fold(a):
        a = jnp.where(mask, a, 0.0)
        return jnp.sum(a[:256].reshape(M, 8, C) + a[256:].reshape(M, 8, C), axis=1)

    numer = fold(acc[...])
    total = fold(jnp.broadcast_to(jnp.sum(tot[...], axis=1, keepdims=True), (SL, C)))
    for i, a in enumerate((numer, total)):
        for rg in range(4):
            for lt in range(2):
                pay[i * 8 + rg * 2 + lt] = a[rg * 8 : rg * 8 + 8, lt * 128 : lt * 128 + 128]
    first = [
        send_small(pay.at[(p + i) % 16], rs.at[p], (h, (p + i) % 16), 6 + i)
        for i in range(1, 16)
    ]
    for t in first:
        t.start()
    rs[p] = pay[p]
    step = weigh_sending(63, 2)
    lax.fori_loop(0, 2, step, 0)
    for t in first:
        t.wait()
    mine[...] = jnp.sum(rs[...], axis=0)
    second = [send_small(mine, hd.at[h], ((h + i) % 8, p), 21 + i) for i in range(1, 8)]
    for t in second:
        t.start()
    hd[h] = mine[...]
    lax.fori_loop(2, 4, step, 0)
    for t in second:
        t.wait()
    pay[0] = jnp.sum(hd[...], axis=0)
    third = [
        send_small(pay.at[0], res.at[p], (h, (p + i) % 16), 28 + i) for i in range(1, 16)
    ]
    for t in third:
        t.start()
    res[p] = pay[0]
    for t in third:
        t.wait()
    send(71, DEVS - 71)

    def gathered(i):
        return jnp.concatenate(
            [
                jnp.concatenate([res[i * 8 + rg * 2], res[i * 8 + rg * 2 + 1]], axis=1)
                for rg in range(4)
            ],
            axis=0,
        )

    stok = gathered(0) / (gathered(1) + 1e-05)
    q, k, v = (nn(stok, wide[i], precision=HI) for i in range(3))

    def spread(a):
        a = jnp.broadcast_to(a[:, None, :], (M, 8, C)).reshape(256, C)
        return jnp.where(mask, jnp.concatenate([a, a], axis=0), 0.0)

    score = nt(spread(k), q, precision=HI) * (1.0 / math.sqrt(DH))
    score = score.reshape(2, M, 8, M)
    e = jnp.exp(score - jnp.max(score, axis=1, keepdims=True))
    att = (e / jnp.sum(e, axis=1, keepdims=True)).reshape(SL, M)
    sout = tn(att, spread(v), precision=HI)
    sout_ref[...] = spread(sout).astype(BF)

    def finish(i):
        o, y, z, g = {}, {}, {}, {}

        def blend(s):
            o[s] = nn(swr[i, s * FSUB : s * FSUB + FSUB, :], sout_ref[...]).astype(BF)

        def norm(s):
            x = rows_in[pl.ds(i * 16, 16)].reshape(BLK, C)[s * FSUB : s * FSUB + FSUB]
            y[s] = x.astype(F32) + nn(o[s], w_e[...]) + b_e[...]
            z[s] = layer_norm(y[s], g2[...], b2[...]).astype(BF)

        def enter(s):
            u = nn(z[s], w_1[...]) + b_1[...]
            g[s] = (u * (1.0 + lax.erf(u * math.sqrt(0.5)))).astype(BF)

        def leave(s):
            a = y[s] + 0.5 * nn(g[s], w_2[...]) + b_2[...]
            at = i * BLK * 2 + s * FSUB * 2
            stage[pl.ds(at, FSUB, stride=2), :] = a[:, :128]
            stage[pl.ds(at + 1, FSUB, stride=2), :] = a[:, 128:]

        skewed(BLK // FSUB, blend, norm, enter, leave)
        rows = pl.ds(i * BLK * 2, BLK * 2)
        pltpu.make_async_copy(stage.at[rows], y_hbm.at[rows], y_sem.at[i]).start()

    def finish_early(i, _):
        finish(i)
        return 0

    def finish_late(i, _):
        arrived(16, row_recv.at[i])
        weigh(i)
        finish(i)
        return 0

    lax.fori_loop(0, EARLY, finish_early, 0)
    lax.fori_loop(EARLY, ROWS // BLK, finish_late, 0)

    n = DEVS - 1
    pltpu.make_async_remote_copy(
        src_ref=xsend.at[pl.ds(0, n)], dst_ref=rows_in.at[pl.ds(0, n)], send_sem=row_send,
        recv_sem=row_recv.at[0], device_id=nbr, device_id_type=MESH,
    ).wait_send()
    pltpu.make_async_remote_copy(
        src_ref=lbl.at[pl.ds(0, n)], dst_ref=lbl_in.at[pl.ds(0, n)], send_sem=lbl_send,
        recv_sem=lbl_recv, device_id=nbr, device_id_type=MESH,
    ).wait()
    for i in range(ROWS // BLK):
        rows = pl.ds(i * BLK * 2, BLK * 2)
        pltpu.make_async_copy(stage.at[rows], y_hbm.at[rows], y_sem.at[i]).wait()


PIECES = 8


def place_kernel(y_hbm, lbl_ref, out_hbm, y, flat, out_v, in_sem, out_sem):
    size = ROWS * 2 // PIECES
    loads = []
    for i in range(PIECES):
        rows = pl.ds(i * size, size)
        loads.append(pltpu.make_async_copy(y_hbm.at[rows], y.at[rows], in_sem.at[i]))
        loads[-1].start()

    def scatter(t, _):
        places = lbl_ref.at[t]
        for r in range(PER):
            flat[pl.ds(places[r], 2), :] = y[pl.ds(t * PER * 2 + 2 * r, 2), :]
        return 0

    for i in range(PIECES):
        loads[i].wait()
        lax.fori_loop(i * DEVS // PIECES, (i + 1) * DEVS // PIECES, scatter, 0, unroll=2)

    def narrow(i, _):
        left = flat[pl.ds(i * 32, 16, stride=2), :]
        right = flat[pl.ds(i * 32 + 1, 16, stride=2), :]
        out_v[pl.ds(i * 16, 16), :] = jnp.concatenate([left, right], axis=1).astype(BF)
        return 0

    stores = []
    for i in range(PIECES):
        lo, hi = i * ROWS // PIECES, (i + 1) * ROWS // PIECES
        lax.fori_loop(lo // 16, hi // 16, narrow, 0, unroll=8)
        rows = pl.ds(lo, hi - lo)
        stores.append(pltpu.make_async_copy(out_v.at[rows], out_hbm.at[rows], out_sem.at[i]))
        stores[-1].start()
    for s in stores:
        s.wait()


VM = pl.BlockSpec(memory_space=pltpu.VMEM)
SM = pl.BlockSpec(memory_space=pltpu.SMEM)
ANY = pl.BlockSpec(memory_space=pl.ANY)
LIMIT = 60 * 1024 * 1024


def exchange(*args):
    dma = pltpu.SemaphoreType.DMA
    return pl.pallas_call(
        exchange_kernel,
        out_shape=[
            jax.ShapeDtypeStruct((ROWS * 2, 128), F32),
            jax.ShapeDtypeStruct((DEVS, 1, 128), jnp.int32),
        ],
        in_specs=[ANY, VM, SM] + [VM] * (len(args) - 3),
        out_specs=[ANY, VM],
        scratch_shapes=[
            pltpu.VMEM((ROWS, C), BF),
            pltpu.VMEM((ROWS * 2, 128), F32),
            pltpu.VMEM((16 * PER * 2, 128), F32),
            pltpu.VMEM((DEVS, PER, C), BF),
            pltpu.VMEM((DEVS, PER, C), BF),
            pltpu.VMEM((DEVS, 1, 128), jnp.int32),
            pltpu.VMEM((DEVS, 128), jnp.int32),
            pltpu.SMEM((DEVS, 128), jnp.int32),
            pltpu.VMEM((SL, BLK), F32),
            pltpu.VMEM((SL, BLK), BF),
            pltpu.VMEM((ROWS // BLK, BLK, SL), BF),
            pltpu.VMEM((BLK, C), BF),
            pltpu.VMEM((SL, C), F32),
            pltpu.VMEM((SL, 128), F32),
            pltpu.VMEM((SL, C), BF),
            pltpu.VMEM((256, 128), F32),
            pltpu.VMEM((3, C, C), F32),
            pltpu.VMEM((16, 8, 128), F32),
            pltpu.VMEM((16, 8, 128), F32),
            pltpu.VMEM((8, 8, 128), F32),
            pltpu.VMEM((8, 128), F32),
            pltpu.VMEM((16, 8, 128), F32),
            pltpu.VMEM((2, 128), F32),
            pltpu.VMEM((8, 2, 128), F32),
            pltpu.VMEM((HEADS, 128), F32),
            pltpu.VMEM((SL, C), BF),
            pltpu.VMEM((ROWS * 2, 128), F32),
            dma, dma, dma((ROWS // BLK,)), dma, dma((8,)), dma, dma, dma((44,)), dma((44,)),
        ],
        compiler_params=pltpu.CompilerParams(
            vmem_limit_bytes=LIMIT, collective_id=0, has_side_effects=True
        ),
        name="exchange",
    )(*args)


def place_rows(y, lbl):
    return pl.pallas_call(
        place_kernel,
        out_shape=jax.ShapeDtypeStruct((ROWS, C), BF),
        in_specs=[ANY, SM],
        out_specs=ANY,
        scratch_shapes=[
            pltpu.VMEM((ROWS * 2, 128), F32),
            pltpu.VMEM((ROWS * 2, 128), F32),
            pltpu.VMEM((ROWS, C), BF),
            pltpu.SemaphoreType.DMA((PIECES,)),
            pltpu.SemaphoreType.DMA((PIECES,)),
        ],
        compiler_params=pltpu.CompilerParams(vmem_limit_bytes=LIMIT),
        name="place_rows",
    )(y, lbl)


def body(
    x, pos, g1, b1, w_f, w_x, part, off, sharp, wq, wk, wv, w_e, b_e, g2, b2, w_1, b_1, w_2, b_2
):
    row = lambda a: a.reshape(1, -1)
    y, lbl = exchange(
        x, pos.reshape(48, 1, 128), sharp, row(g1),
        row(b1), w_f, w_x, part, row(off), wq, wk, wv, w_e, row(b_e), row(g2), row(b2), w_1,
        row(b_1), w_2, row(b_2),
    )
    return place_rows(y, lbl.reshape(DEVS, 128))[None]


def solution(mesh):
    both = ("head", "pts")
    in_specs = (P(both, None), P(both)) + (P(),) * 6 + (P("head"),) + (P(),) * 11
    return jax.shard_map(
        body, mesh=mesh, in_specs=in_specs, out_specs=P("pts", "head", None), check_vma=False
    )
```
